256 devices in a mesh: sub: 4 (over z_hi, core), gx: 64 (over x, z_lo, y).
Axes of the slice: x: 4, y: 4, z: 8 (z_hi: 2, z_lo: 4; z = z_hi * 4 + z_lo), core: 2. Of those that a mesh axis runs over, the one named last changes fastest.
Arguments:
- value_field: float32 [8, 512, 256, 256], P('sub', 'gx'), may hold values from -6 to 6
- speed_field: float32 [8, 512, 256, 256], P('sub', 'gx'), may hold values from 0.25 to 2
- drift_matrix: float32 [8, 3, 3], P('sub'), may hold values from -0.5 to 0.5
- drift_offset: float32 [8, 3], P('sub'), may hold values from -0.5 to 0.5
- control_bound: float32 [8, 3], P('sub'), may hold values from 0.5 to 1
- partner_table: int32 [8], replicated, may hold values from 0 to 7, as said below
- dropped_dim: int32 [8], P('sub'), may hold values from 1 to 2, as said below
Outputs:
- final_value: float32 [8, 512, 256, 256], P('sub', 'gx')
- shared_plane: float32 [8, 512, 256], P('sub', 'gx')
The draws below stay inside these ranges and needn't reach their ends.
Inputs may be any that keep to these rules, and one draw needn't show every extreme that they name: `partner_table`: a permutation of the 8 subsystems that forms a single cycle through all of them, so no subsystem is its own partner. `dropped_dim`: half of the subsystems drop dimension 1 and half dimension 2.
All inputs are finite; a program needn't handle non-finite values.
Results may differ from the reference program's by a relative error of at most 0.00075.
Values sent between devices are 32-bit elements; how exact they have to be, the bound alone decides.
A program may use at most 128 MiB of HBM per device.

```python
import math
import jax
import jax.numpy as jnp
from jax import lax

N = 256
STEPS = 2
SUBS = 8
NX = 512


def draw_partner_table(key, part):
    order = jax.random.permutation(jax.random.fold_in(key, 11), SUBS).astype(jnp.int32)
    table = jnp.zeros((SUBS,), jnp.int32).at[order].set(jnp.roll(order, -1))
    return table.astype(jnp.int32)


def draw_dropped_dim(key, part):
    order = jax.random.permutation(jax.random.fold_in(key, 23), SUBS).astype(jnp.int32)
    return (1 + order % 2).astype(jnp.int32)


def steps_of(own_key, shape, pieces, least, high):
    loudness = 1.0
    for axis_at, blocks in pieces:
        draws = jax.random.uniform(jax.random.fold_in(jax.random.fold_in(own_key, 6), axis_at), (blocks,), jnp.float32, least / len(pieces), high / len(pieces))
        loudness = loudness * jnp.repeat(jnp.exp(draws), shape[axis_at] // blocks).reshape((-1,) + (1,) * (len(shape) - 1 - axis_at))
    return loudness


def gaussian(key, extent, scale, most, cuts=(), kind=jnp.bfloat16):
    loudness = steps_of(key, extent, cuts, -0.22, 0.18) if cuts else 1.0
    result = jax.random.normal(key, extent, jnp.float32) * scale * loudness
    return jnp.minimum(jnp.maximum(result, -most), most).astype(kind)


def setup_inputs(seed: int = 0) -> dict:
    key_list = jax.random.split(jax.random.key(seed), 8)
    value_field = gaussian(key_list[0], (SUBS, NX, N, N), 1.0, 6.0, ((0, 4), (1, 64)), jnp.float32)
    speed_field = jnp.clip(jnp.exp(math.log(2.0) - 2.0794415 * jax.random.uniform(key_list[1], (SUBS, NX, N, N), jnp.float32) ** steps_of(key_list[1], (SUBS, NX, N, N), ((0, 4), (1, 64)), -0.2, 0.2)), 0.25, 2.0)
    drift_matrix = jnp.clip(jax.random.uniform(key_list[2], (SUBS, 3, 3), jnp.float32, -0.5, 0.5) * steps_of(key_list[2], (SUBS, 3, 3), ((0, 4),), -0.4, 0.0), -0.5, 0.5)
    drift_offset = jnp.clip(jax.random.uniform(key_list[3], (SUBS, 3), jnp.float32, -0.5, 0.5) * steps_of(key_list[3], (SUBS, 3), ((0, 4),), -0.4, 0.0), -0.5, 0.5)
    control_bound = jnp.clip(0.5 + 0.5 * jax.random.uniform(key_list[4], (SUBS, 3), jnp.float32) ** steps_of(key_list[4], (SUBS, 3), ((0, 4),), -0.2, 0.2), 0.5, 1.0)
    partner_table = draw_partner_table(jax.random.fold_in(key_list[7], 71), 0)
    dropped_dim = draw_dropped_dim(jax.random.fold_in(key_list[7], 71), 0)
    return {"value_field": value_field, "speed_field": speed_field, "drift_matrix": drift_matrix, "drift_offset": drift_offset, "control_bound": control_bound, "partner_table": partner_table, "dropped_dim": dropped_dim}


def smaller(first, second):
    return jnp.where(jnp.abs(first) <= jnp.abs(second), first, second)


def one_sided(extended, dim_index, step_size):
    cell_count = extended.shape[dim_index] - 4

    def shifted(offset):
        return lax.slice_in_dim(extended, 2 + offset, 2 + offset + cell_count, axis=dim_index)

    back_two = shifted(-2)
    back_one = shifted(-1)
    middle = shifted(0)
    ahead_one = shifted(1)
    ahead_two = shifted(2)
    curve_back = back_two - 2.0 * back_one + middle
    curve_mid = back_one - 2.0 * middle + ahead_one
    curve_ahead = middle - 2.0 * ahead_one + ahead_two
    minus_side = (middle - back_one) / step_size + smaller(curve_back, curve_mid) / (2.0 * step_size)
    plus_side = (ahead_one - middle) / step_size - smaller(curve_mid, curve_ahead) / (2.0 * step_size)
    return minus_side, plus_side


def coordinates(first_row, cell_count, total_cells):
    indices = (first_row + jnp.arange(cell_count, dtype=jnp.int32)) % total_cells
    return -1.0 + (indices.astype(jnp.float32) + 0.5) * (2.0 / total_cells)


def advance(extended, speed_rows, first_coords, drift_matrix, drift_offset, control_bound, spacing, time_step):
    row_count = extended.shape[1] - 4
    grid_cells = extended.shape[2]
    center = lax.slice_in_dim(extended, 2, 2 + row_count, axis=1)
    gradients = [one_sided(extended, 1, spacing[0])]
    padded = jnp.pad(center, ((0, 0), (0, 0), (2, 2), (0, 0)), mode="edge")
    gradients.append(one_sided(padded, 2, spacing[1]))
    padded = jnp.pad(center, ((0, 0), (0, 0), (0, 0), (2, 2)), mode="edge")
    gradients.append(one_sided(padded, 3, spacing[2]))
    second_axis = coordinates(0, grid_cells, grid_cells)
    third_axis = coordinates(0, extended.shape[3], extended.shape[3])
    positions = (first_coords[None, :, None, None], second_axis[None, None, :, None], third_axis[None, None, None, :])
    hamiltonian = jnp.zeros_like(center)
    for d in range(3):
        drift_term = drift_offset[:, d][:, None, None, None]
        for e in range(3):
            drift_term = drift_term + drift_matrix[:, d, e][:, None, None, None] * positions[e]
        minus_side, plus_side = gradients[d]
        average = 0.5 * (minus_side + plus_side)
        reach = control_bound[:, d][:, None, None, None] * speed_rows
        hamiltonian = hamiltonian + drift_term * average - reach * jnp.abs(average) - (jnp.abs(drift_term) + reach) * 0.5 * (plus_side - minus_side)
    return jnp.minimum(center, center - time_step * hamiltonian)


def reference(value_field, speed_field, drift_matrix, drift_offset, control_bound, partner_table, dropped_dim):
    spacing = (2.0 / NX, 2.0 / N, 2.0 / N)
    time_step = min(spacing) / 15.0
    first_coords = coordinates(0, NX, NX)
    current = value_field
    for repeat in range(STEPS):
        extended = jnp.pad(current, ((0, 0), (2, 2), (0, 0), (0, 0)), mode="wrap")
        current = advance(extended, speed_field, first_coords, drift_matrix, drift_offset, control_bound, spacing, time_step)
    min_second = jnp.min(current, axis=2)
    min_third = jnp.min(current, axis=3)
    own_plane = jnp.where((dropped_dim == 1)[:, None, None], min_second, min_third)
    partner_plane = own_plane[partner_table]
    return current, jnp.maximum(own_plane, partner_plane)
```

```python
import functools

import jax
import jax.numpy as jnp
from jax import lax
from jax.experimental import pallas as pl
from jax.experimental.pallas import tpu as pltpu
from jax.sharding import PartitionSpec as P

STEPS = 2
LANES = 128
PAD = 8
TS = 16
BLOCKS = 4


def pick(a, abs_a, b, abs_b):
    return jnp.where(abs_a <= abs_b, a, b)


def kernel(
    dims,
    value_hbm,
    speed_hbm,
    matrix_hbm,
    offset_hbm,
    bound_hbm,
    partner_hbm,
    dropped_hbm,
    final,
    shared_ref,
    first,
    second,
    speed,
    drift_matrix,
    drift_offset,
    control_bound,
    partner_table,
    dropped_dim,
    low_second,
    low_third,
    own,
    gathered,
    load_sem,
    scalar_sem,
    send_sem,
    recv_sem,
    plane_send,
    plane_recv,
):
    subs, rows, cells, halves, sub_count, ring, total_rows = dims
    block = cells // BLOCKS
    chunks = subs * BLOCKS
    sub_at = lax.axis_index("sub")
    at = lax.axis_index("gx")
    right = lax.rem(at + 1, ring)
    left = lax.rem(at + ring - 1, ring)
    peers = [lax.rem(sub_at + k, sub_count) for k in range(1, sub_count)]

    spacing = (2.0 / total_rows, 2.0 / cells, 2.0 / (halves * LANES))
    time_step = min(spacing) / 15.0
    scale = tuple(time_step / (2.0 * h) for h in spacing)

    barrier = pltpu.get_barrier_semaphore()
    for target in (left, right):
        pl.semaphore_signal(barrier, inc=1, device_id={"gx": target}, device_id_type=pl.DeviceIdType.MESH)
    for target in peers:
        pl.semaphore_signal(barrier, inc=1, device_id={"sub": target}, device_id_type=pl.DeviceIdType.MESH)

    def loads():
        out = []
        for s in range(subs):
            for h in range(halves):
                lanes = pl.ds(h * LANES, LANES)
                out.append(
                    pltpu.make_async_copy(
                        value_hbm.at[s, :, :, lanes],
                        first.at[s, pl.ds(2, rows), h, pl.ds(PAD, cells), :],
                        load_sem.at[0, s, h],
                    )
                )
                out.append(
                    pltpu.make_async_copy(
                        speed_hbm.at[s, :, :, lanes], speed.at[s, :, h], load_sem.at[1, s, h]
                    )
                )
        for k, (source, held) in enumerate(
            (
                (matrix_hbm, drift_matrix),
                (offset_hbm, drift_offset),
                (bound_hbm, control_bound),
                (partner_hbm, partner_table),
                (dropped_hbm, dropped_dim),
            )
        ):
            out.append(pltpu.make_async_copy(source, held, scalar_sem.at[k]))
        return out

    for copy in loads():
        copy.start()
    pl.semaphore_wait(barrier, 2 + len(peers))

    def rim_copies(step, chunk):
        s = chunk // BLOCKS
        j = lax.rem(chunk, BLOCKS) * block
        out = []
        for way, (source_row, target_row, target) in enumerate(
            ((rows - 2, 0, right), (0, rows + 2, left))
        ):
            for h in range(halves):
                if step == 0:
                    source = value_hbm.at[
                        s, pl.ds(source_row, 2), pl.ds(j, block), pl.ds(h * LANES, LANES)
                    ]
                    held = first
                else:
                    source = second.at[s, pl.ds(source_row + 2, 2), h, pl.ds(PAD + j, block), :]
                    held = second
                out.append(
                    pltpu.make_async_remote_copy(
                        src_ref=source,
                        dst_ref=held.at[s, pl.ds(target_row, 2), h, pl.ds(PAD + j, block), :],
                        send_sem=send_sem.at[step, way, chunk, h],
                        recv_sem=recv_sem.at[step, way, chunk, h],
                        device_id={"gx": target},
                        device_id_type=pl.DeviceIdType.MESH,
                    )
                )
        return out

    @pl.loop(0, chunks)
    def _(chunk):
        for copy in rim_copies(0, chunk):
            copy.start()

    for copy in loads():
        copy.wait()

    def repeat_ends(held):
        @pl.loop(0, subs * rows)
        def _(i):
            s = i // rows
            r = lax.rem(i, rows) + 2
            for h in range(halves):
                for cell, start in ((PAD, PAD - 2), (PAD + cells - 1, PAD + cells)):
                    held[s, r, h, pl.ds(start, 2), :] = jnp.broadcast_to(
                        held[s, r, h, pl.ds(cell, 1), :], (2, LANES)
                    )

    repeat_ends(first)
    lane = lax.broadcasted_iota(jnp.int32, (TS, LANES), 1)
    at_start = lane == 0
    at_end = lane == LANES - 1
    low_third[...] = jnp.zeros_like(low_third)
    low_second[...] = jnp.full_like(low_second, jnp.inf)

    def coordinate(index, total):
        return -1.0 + (index.astype(jnp.float32) + 0.5) * (2.0 / total)

    def ahead(parts, edge):
        turned = [pltpu.roll(p, LANES - 1, 1) for p in parts]
        return [
            jnp.where(at_end, turned[h + 1] if h + 1 < halves else edge, turned[h])
            for h in range(halves)
        ]

    def behind(parts, edge):
        turned = [pltpu.roll(p, 1, 1) for p in parts]
        return [
            jnp.where(at_start, turned[h - 1] if h > 0 else edge, turned[h]) for h in range(halves)
        ]

    def cells_of(held, step, s, groups, start):
        matrix = [[drift_matrix[d, s, e] * scale[d] for e in range(3)] for d in range(3)]
        offset = [drift_offset[s, d] * scale[d] for d in range(3)]
        bound = [control_bound[s, d] * scale[d] for d in range(3)]
        index = start + lax.broadcasted_iota(jnp.int32, (TS, LANES), 0)
        second_axis = coordinate(index, cells)
        drift_base = []
        for h in range(halves):
            third_axis = coordinate(lane + h * LANES, halves * LANES)
            drift_base.append(
                [matrix[d][1] * second_axis + matrix[d][2] * third_axis for d in range(3)]
            )
        lows = None
        for low_row, high_row in groups:

            def value(r, h, shift=0):
                return held[s, r + 2, h, pl.ds(PAD + start + shift, TS), :]

            middle = {r: [value(r, h) for h in range(halves)] for r in range(low_row - 2, high_row + 2)}
            along_first = {}
            for h in range(halves):
                slope = {r: middle[r + 1][h] - middle[r][h] for r in range(low_row - 2, high_row + 1)}
                curve = {r: slope[r] - slope[r - 1] for r in range(low_row - 1, high_row + 1)}
                size = {r: jnp.abs(curve[r]) for r in curve}
                for r in range(low_row - 1, high_row):
                    face = pick(curve[r], size[r], curve[r + 1], size[r + 1])
                    twice = slope[r] + slope[r]
                    along_first[r, h, 0] = twice - face
                    along_first[r + 1, h, 1] = -(twice + face)
            for r in range(low_row, high_row):
                x0 = -1.0 + ((at * rows + r).astype(jnp.float32) + 0.5) * (2.0 / total_rows)
                center = middle[r]
                up = ahead(center, center[halves - 1])
                down = behind(center, center[0])
                plus = [up[h] - center[h] for h in range(halves)]
                minus = [down[h] - center[h] for h in range(halves)]
                curve = [plus[h] + minus[h] for h in range(halves)]
                curve_up = ahead(curve, 0.0)
                curve_down = behind(curve, 0.0)
                results = []
                for h in range(halves):
                    sides = [(along_first[r, h, 0], along_first[r, h, 1])]
                    a2, a1, b1, b2 = (value(r, h, k) for k in (-2, -1, 1, 2))
                    p = b1 - center[h]
                    m = a1 - center[h]
                    c = p + m
                    c_up = (b2 - b1) - p
                    c_down = (a2 - a1) - m
                    size, size_up, size_down = jnp.abs(c), jnp.abs(c_up), jnp.abs(c_down)
                    sides.append(
                        (
                            (p + p) - pick(c, size, c_up, size_up),
                            (m + m) - pick(c_down, size_down, c, size),
                        )
                    )
                    c, c_up, c_down = curve[h], curve_up[h], curve_down[h]
                    size, size_up, size_down = jnp.abs(c), jnp.abs(c_up), jnp.abs(c_down)
                    sides.append(
                        (
                            (plus[h] + plus[h]) - pick(c, size, c_up, size_up),
                            (minus[h] + minus[h]) - pick(c_down, size_down, c, size),
                        )
                    )
                    drifting = None
                    reaching = None
                    for d, (x, y) in enumerate(sides):
                        drift = drift_base[h][d] + (offset[d] + matrix[d][0] * x0)
                        term = jnp.abs(drift) * jnp.where(drift >= 0.0, y, x)
                        reach = bound[d] * jnp.maximum(x, y)
                        drifting = term if drifting is None else drifting + term
                        reaching = reach if reaching is None else reaching + reach
                    gain = drifting + speed[s, r, h, pl.ds(start, TS), :] * reaching
                    result = center[h] + jnp.minimum(gain, 0.0)
                    results.append(result)
                    if step == 0:
                        second[s, r + 2, h, pl.ds(PAD + start, TS), :] = result
                    else:
                        final[s, r, pl.ds(start, TS), pl.ds(h * LANES, LANES)] = result
                        low = result[:8]
                        for k in range(8, TS, 8):
                            low = jnp.minimum(low, result[k : k + 8])
                        low_second[s, r, h] = jnp.minimum(low_second[s, r, h], low)
                if step == 1:
                    joint = results[0]
                    for part in results[1:]:
                        joint = jnp.minimum(joint, part)
                    least = jnp.min(joint, axis=1, keepdims=True)
                    if lows is None:
                        lows = low_third[s, pl.ds(start, TS), :]
                    lows = jnp.where(lane == r, least, lows)
        if step == 1:
            low_third[s, pl.ds(start, TS), :] = lows

    def run(held, step, chunk, groups):
        s = chunk // BLOCKS
        j = lax.rem(chunk, BLOCKS) * block

        @pl.loop(0, block // TS)
        def _(t):
            cells_of(held, step, s, groups, pl.multiple_of(j + t * TS, TS))

    inner = ((2, rows - 2),)
    rims = ((0, 2), (rows - 2, rows))

    @pl.loop(0, chunks)
    def _(chunk):
        run(first, 0, chunk, inner)
        for copy in rim_copies(0, chunk):
            copy.wait_recv()
        run(first, 0, chunk, rims)
        for copy in rim_copies(1, chunk):
            copy.start()

    repeat_ends(second)

    @pl.loop(0, chunks)
    def _(chunk):
        run(second, 1, chunk, inner)
        for copy in rim_copies(1, chunk):
            copy.wait_recv()
        run(second, 1, chunk, rims)

    for s in range(subs):
        over_third = jnp.transpose(low_third[s])[:rows]
        for h in range(halves):
            over_second = jnp.min(low_second[s, :, h], axis=1)
            plane = jnp.where(
                dropped_dim[s] == 1, over_second, over_third[:, h * LANES : (h + 1) * LANES]
            )
            own[s, :, pl.ds(h * LANES, LANES)] = plane
            gathered[sub_at * subs + s, :, pl.ds(h * LANES, LANES)] = plane

    plane_copies = [
        pltpu.make_async_remote_copy(
            src_ref=own,
            dst_ref=gathered.at[pl.ds(sub_at * subs, subs)],
            send_sem=plane_send.at[k],
            recv_sem=plane_recv.at[k],
            device_id={"sub": target},
            device_id_type=pl.DeviceIdType.MESH,
        )
        for k, target in enumerate(peers)
    ]
    for copy in plane_copies:
        copy.start()

    @pl.loop(0, chunks)
    def _(chunk):
        for step in range(STEPS):
            for copy in rim_copies(step, chunk):
                copy.wait_send()

    for copy in plane_copies:
        copy.wait_recv()
    for s in range(subs):
        partner = partner_table[sub_at * subs + s]
        shared_ref[s] = jnp.maximum(own[s], gathered[partner])
    for copy in plane_copies:
        copy.wait_send()


def on_device(dims, value_field, speed_field, drift_matrix, *others):
    subs, rows, cells, halves, sub_count, ring, total_rows = dims
    chunks = subs * BLOCKS
    in_vmem = pl.BlockSpec(memory_space=pltpu.VMEM)
    held = pltpu.VMEM((subs, rows + 4, halves, cells + 2 * PAD, LANES), jnp.float32)
    whole = pltpu.VMEM((subs, rows, halves, cells, LANES), jnp.float32)
    return pl.pallas_call(
        functools.partial(kernel, dims),
        out_shape=(
            jax.ShapeDtypeStruct((subs, rows, cells, halves * LANES), jnp.float32),
            jax.ShapeDtypeStruct((subs, rows, cells), jnp.float32),
        ),
        in_specs=[pl.BlockSpec(memory_space=pltpu.HBM)] * 7,
        out_specs=(in_vmem, in_vmem),
        scratch_shapes=[
            held,
            held,
            whole,
            pltpu.SMEM((3, subs, 3), jnp.float32),
            pltpu.SMEM((subs, 3), jnp.float32),
            pltpu.SMEM((subs, 3), jnp.float32),
            pltpu.SMEM((sub_count * subs,), jnp.int32),
            pltpu.SMEM((subs,), jnp.int32),
            pltpu.VMEM((subs, rows, halves, 8, LANES), jnp.float32),
            pltpu.VMEM((subs, cells, LANES), jnp.float32),
            pltpu.VMEM((subs, rows, cells), jnp.float32),
            pltpu.VMEM((sub_count * subs, rows, cells), jnp.float32),
            pltpu.SemaphoreType.DMA((2, subs, halves)),
            pltpu.SemaphoreType.DMA((5,)),
            pltpu.SemaphoreType.DMA((STEPS, 2, chunks, halves)),
            pltpu.SemaphoreType.DMA((STEPS, 2, chunks, halves)),
            pltpu.SemaphoreType.DMA((sub_count - 1,)),
            pltpu.SemaphoreType.DMA((sub_count - 1,)),
        ],
        compiler_params=pltpu.CompilerParams(
            collective_id=0, has_side_effects=True, vmem_limit_bytes=48 * 1024 * 1024
        ),
        name="steps_and_planes",
    )(value_field, speed_field, jnp.transpose(drift_matrix, (1, 0, 2)), *others)


def solution(mesh):
    sub_count, ring = mesh.shape["sub"], mesh.shape["gx"]

    def whole(value_field, *others):
        total_subs, total_rows, cells, third = value_field.shape
        dims = (
            total_subs // sub_count,
            total_rows // ring,
            cells,
            third // LANES,
            sub_count,
            ring,
            total_rows,
        )
        step = jax.shard_map(
            functools.partial(on_device, dims),
            mesh=mesh,
            in_specs=(
                P("sub", "gx", None, None),
                P("sub", "gx", None, None),
                P("sub", None, None),
                P("sub", None),
                P("sub", None),
                P(),
                P("sub"),
            ),
            out_specs=(P("sub", "gx", None, None), P("sub", "gx", None)),
            check_vma=False,
        )
        return step(value_field, *others)

    return whole
```

```python
import functools

import jax
import jax.numpy as jnp
from jax import lax
from jax.experimental import pallas as pl
from jax.experimental.pallas import tpu as pltpu
from jax.sharding import PartitionSpec as P

STEPS = 2
LANES = 128
PAD = 8
TS = 16
BLOCKS = 8


def pick(a, abs_a, b, abs_b):
    return jnp.where(abs_a <= abs_b, a, b)


def kernel(
    dims,
    value_hbm,
    speed_hbm,
    matrix_hbm,
    offset_hbm,
    bound_hbm,
    partner_hbm,
    dropped_hbm,
    final,
    shared_ref,
    first,
    second,
    speed,
    drift_matrix,
    drift_offset,
    control_bound,
    partner_table,
    dropped_dim,
    low_second,
    low_third,
    own,
    gathered,
    load_sem,
    scalar_sem,
    send_sem,
    recv_sem,
    plane_send,
    plane_recv,
):
    subs, rows, cells, halves, sub_count, ring, total_rows = dims
    block = cells // BLOCKS
    chunks = subs * BLOCKS
    sub_at = lax.axis_index("sub")
    at = lax.axis_index("gx")
    right = lax.rem(at + 1, ring)
    left = lax.rem(at + ring - 1, ring)
    peers = [lax.rem(sub_at + k, sub_count) for k in range(1, sub_count)]

    spacing = (2.0 / total_rows, 2.0 / cells, 2.0 / (halves * LANES))
    time_step = min(spacing) / 15.0
    scale = tuple(time_step / (2.0 * h) for h in spacing)

    barrier = pltpu.get_barrier_semaphore()
    for target in (left, right):
        pl.semaphore_signal(barrier, inc=1, device_id={"gx": target}, device_id_type=pl.DeviceIdType.MESH)
    for target in peers:
        pl.semaphore_signal(barrier, inc=1, device_id={"sub": target}, device_id_type=pl.DeviceIdType.MESH)

    def loads(source, held, first_row, pad, kind):
        return [
            pltpu.make_async_copy(
                source.at[s, :, :, pl.ds(h * LANES, LANES)],
                held.at[s, pl.ds(first_row, rows), h, pl.ds(pad, cells), :],
                load_sem.at[kind, s, h],
            )
            for s in range(subs)
            for h in range(halves)
        ]

    value_loads = loads(value_hbm, first, 2, PAD, 0)
    other_loads = loads(speed_hbm, speed, 0, 0, 1) + [
        pltpu.make_async_copy(source, held, scalar_sem.at[k])
        for k, (source, held) in enumerate(
            (
                (matrix_hbm, drift_matrix),
                (offset_hbm, drift_offset),
                (bound_hbm, control_bound),
                (partner_hbm, partner_table),
                (dropped_hbm, dropped_dim),
            )
        )
    ]
    for copy in value_loads + other_loads:
        copy.start()
    pl.semaphore_wait(barrier, 2 + len(peers))

    def rim_copies(step, chunk):
        s = chunk // BLOCKS
        j = lax.rem(chunk, BLOCKS) * block
        out = []
        for way, (source_row, target_row, target) in enumerate(
            ((rows - 2, 0, right), (0, rows + 2, left))
        ):
            held = first if step == 0 else second
            cells_sent = pl.ds(PAD + j, block)
            out.append(
                pltpu.make_async_remote_copy(
                    src_ref=held.at[s, pl.ds(source_row + 2, 2), :, cells_sent, :],
                    dst_ref=held.at[s, pl.ds(target_row, 2), :, cells_sent, :],
                    send_sem=send_sem.at[step, way, chunk],
                    recv_sem=recv_sem.at[step, way, chunk],
                    device_id={"gx": target},
                    device_id_type=pl.DeviceIdType.MESH,
                )
            )
        return out

    for copy in value_loads:
        copy.wait()

    @pl.loop(0, chunks)
    def _(chunk):
        for copy in rim_copies(0, chunk):
            copy.start()

    for copy in other_loads:
        copy.wait()

    def repeat_ends(held):
        @pl.loop(0, subs * rows)
        def _(i):
            s = i // rows
            r = lax.rem(i, rows) + 2
            for h in range(halves):
                for cell, start in ((PAD, PAD - 2), (PAD + cells - 1, PAD + cells)):
                    held[s, r, h, pl.ds(start, 2), :] = jnp.broadcast_to(
                        held[s, r, h, pl.ds(cell, 1), :], (2, LANES)
                    )

    repeat_ends(first)
    lane = lax.broadcasted_iota(jnp.int32, (TS, LANES), 1)
    at_start = lane == 0
    at_end = lane == LANES - 1
    low_third[...] = jnp.zeros_like(low_third)
    low_second[...] = jnp.full_like(low_second, jnp.inf)

    def coordinate(index, total):
        return -1.0 + (index.astype(jnp.float32) + 0.5) * (2.0 / total)

    def ahead(parts, edge):
        turned = [pltpu.roll(p, LANES - 1, 1) for p in parts]
        return [
            jnp.where(at_end, turned[h + 1] if h + 1 < halves else edge, turned[h])
            for h in range(halves)
        ]

    def behind(parts, edge):
        turned = [pltpu.roll(p, 1, 1) for p in parts]
        return [
            jnp.where(at_start, turned[h - 1] if h > 0 else edge, turned[h]) for h in range(halves)
        ]

    def cells_of(held, step, s, groups, start):
        matrix = [[drift_matrix[d, s, e] * scale[d] for e in range(3)] for d in range(3)]
        offset = [drift_offset[s, d] * scale[d] for d in range(3)]
        bound = [control_bound[s, d] * scale[d] for d in range(3)]
        index = start + lax.broadcasted_iota(jnp.int32, (TS, LANES), 0)
        second_axis = coordinate(index, cells)
        drift_base = []
        for h in range(halves):
            third_axis = coordinate(lane + h * LANES, halves * LANES)
            drift_base.append(
                [matrix[d][1] * second_axis + matrix[d][2] * third_axis for d in range(3)]
            )
        lows = None
        for low_row, high_row in groups:

            def value(r, h, shift=0):
                return held[s, r + 2, h, pl.ds(PAD + start + shift, TS), :]

            middle = {r: [value(r, h) for h in range(halves)] for r in range(low_row - 2, high_row + 2)}
            along_first = {}
            for h in range(halves):
                slope = {r: middle[r + 1][h] - middle[r][h] for r in range(low_row - 2, high_row + 1)}
                curve = {r: slope[r] - slope[r - 1] for r in range(low_row - 1, high_row + 1)}
                size = {r: jnp.abs(curve[r]) for r in curve}
                for r in range(low_row - 1, high_row):
                    face = pick(curve[r], size[r], curve[r + 1], size[r + 1])
                    twice = slope[r] + slope[r]
                    along_first[r, h, 0] = twice - face
                    along_first[r + 1, h, 1] = -(twice + face)
            for r in range(low_row, high_row):
                x0 = -1.0 + ((at * rows + r).astype(jnp.float32) + 0.5) * (2.0 / total_rows)
                center = middle[r]
                up = ahead(center, center[halves - 1])
                down = behind(center, center[0])
                plus = [up[h] - center[h] for h in range(halves)]
                minus = [down[h] - center[h] for h in range(halves)]
                curve = [plus[h] + minus[h] for h in range(halves)]
                curve_up = ahead(curve, 0.0)
                curve_down = behind(curve, 0.0)
                results = []
                for h in range(halves):
                    sides = [(along_first[r, h, 0], along_first[r, h, 1])]
                    a2, a1, b1, b2 = (value(r, h, k) for k in (-2, -1, 1, 2))
                    p = b1 - center[h]
                    m = a1 - center[h]
                    c = p + m
                    c_up = (b2 - b1) - p
                    c_down = (a2 - a1) - m
                    size, size_up, size_down = jnp.abs(c), jnp.abs(c_up), jnp.abs(c_down)
                    sides.append(
                        (
                            (p + p) - pick(c, size, c_up, size_up),
                            (m + m) - pick(c_down, size_down, c, size),
                        )
                    )
                    c, c_up, c_down = curve[h], curve_up[h], curve_down[h]
                    size, size_up, size_down = jnp.abs(c), jnp.abs(c_up), jnp.abs(c_down)
                    sides.append(
                        (
                            (plus[h] + plus[h]) - pick(c, size, c_up, size_up),
                            (minus[h] + minus[h]) - pick(c_down, size_down, c, size),
                        )
                    )
                    drifting = None
                    reaching = None
                    for d, (x, y) in enumerate(sides):
                        drift = drift_base[h][d] + (offset[d] + matrix[d][0] * x0)
                        term = jnp.abs(drift) * jnp.where(drift >= 0.0, y, x)
                        reach = bound[d] * jnp.maximum(x, y)
                        drifting = term if drifting is None else drifting + term
                        reaching = reach if reaching is None else reaching + reach
                    gain = drifting + speed[s, r, h, pl.ds(start, TS), :] * reaching
                    result = center[h] + jnp.minimum(gain, 0.0)
                    results.append(result)
                    if step == 0:
                        second[s, r + 2, h, pl.ds(PAD + start, TS), :] = result
                    else:
                        final[s, r, pl.ds(start, TS), pl.ds(h * LANES, LANES)] = result
                        low = result[:8]
                        for k in range(8, TS, 8):
                            low = jnp.minimum(low, result[k : k + 8])
                        low_second[s, r, h] = jnp.minimum(low_second[s, r, h], low)
                if step == 1:
                    joint = results[0]
                    for part in results[1:]:
                        joint = jnp.minimum(joint, part)
                    least = jnp.min(joint, axis=1, keepdims=True)
                    if lows is None:
                        lows = low_third[s, pl.ds(start, TS), :]
                    lows = jnp.where(lane == r, least, lows)
        if step == 1:
            low_third[s, pl.ds(start, TS), :] = lows

    def run(held, step, chunk, groups):
        s = chunk // BLOCKS
        j = lax.rem(chunk, BLOCKS) * block

        @pl.loop(0, block // TS)
        def _(t):
            cells_of(held, step, s, groups, pl.multiple_of(j + t * TS, TS))

    inner = ((2, rows - 2),)
    rims = ((0, 2), (rows - 2, rows))

    @pl.loop(0, chunks)
    def _(chunk):
        run(first, 0, chunk, inner)
        for copy in rim_copies(0, chunk):
            copy.wait_recv()
        run(first, 0, chunk, rims)
        for copy in rim_copies(1, chunk):
            copy.start()

    repeat_ends(second)

    @pl.loop(0, chunks)
    def _(chunk):
        run(second, 1, chunk, inner)
        for copy in rim_copies(1, chunk):
            copy.wait_recv()
        run(second, 1, chunk, rims)

    for s in range(subs):
        over_third = jnp.transpose(low_third[s])[:rows]
        for h in range(halves):
            over_second = jnp.min(low_second[s, :, h], axis=1)
            plane = jnp.where(
                dropped_dim[s] == 1, over_second, over_third[:, h * LANES : (h + 1) * LANES]
            )
            own[s, :, pl.ds(h * LANES, LANES)] = plane
            gathered[sub_at * subs + s, :, pl.ds(h * LANES, LANES)] = plane

    plane_copies = [
        pltpu.make_async_remote_copy(
            src_ref=own,
            dst_ref=gathered.at[pl.ds(sub_at * subs, subs)],
            send_sem=plane_send.at[k],
            recv_sem=plane_recv.at[k],
            device_id={"sub": target},
            device_id_type=pl.DeviceIdType.MESH,
        )
        for k, target in enumerate(peers)
    ]
    for copy in plane_copies:
        copy.start()

    @pl.loop(0, chunks)
    def _(chunk):
        for step in range(STEPS):
            for copy in rim_copies(step, chunk):
                copy.wait_send()

    for copy in plane_copies:
        copy.wait_recv()
    for s in range(subs):
        partner = partner_table[sub_at * subs + s]
        shared_ref[s] = jnp.maximum(own[s], gathered[partner])
    for copy in plane_copies:
        copy.wait_send()


def put_out(final, shared, final_out, shared_out, final_sem, shared_sem):
    subs, rows = final.shape[:2]
    pieces = final_sem.shape[1]
    count = rows // pieces
    copies = [pltpu.make_async_copy(shared, shared_out, shared_sem)]
    for s in range(subs):
        for k in range(pieces):
            at = (s, pl.ds(k * count, count))
            copies.append(pltpu.make_async_copy(final.at[at], final_out.at[at], final_sem.at[s, k]))
    for copy in copies:
        copy.start()
    for copy in copies:
        copy.wait()


def on_device(dims, value_field, speed_field, drift_matrix, *others):
    subs, rows, cells, halves, sub_count, ring, total_rows = dims
    chunks = subs * BLOCKS
    in_vmem = pl.BlockSpec(memory_space=pltpu.VMEM)
    held = pltpu.VMEM((subs, rows + 4, halves, cells + 2 * PAD, LANES), jnp.float32)
    whole = pltpu.VMEM((subs, rows, halves, cells, LANES), jnp.float32)
    arrays = (value_field, speed_field, jnp.transpose(drift_matrix, (1, 0, 2)), *others)
    results = pl.pallas_call(
        functools.partial(kernel, dims),
        out_shape=(
            jax.ShapeDtypeStruct((subs, rows, cells, halves * LANES), jnp.float32),
            jax.ShapeDtypeStruct((subs, rows, cells), jnp.float32),
        ),
        in_specs=[pl.BlockSpec(memory_space=pltpu.HBM)] * 7,
        out_specs=(in_vmem, in_vmem),
        scratch_shapes=[
            held,
            held,
            whole,
            pltpu.SMEM((3, subs, 3), jnp.float32),
            pltpu.SMEM((subs, 3), jnp.float32),
            pltpu.SMEM((subs, 3), jnp.float32),
            pltpu.SMEM((sub_count * subs,), jnp.int32),
            pltpu.SMEM((subs,), jnp.int32),
            pltpu.VMEM((subs, rows, halves, 8, LANES), jnp.float32),
            pltpu.VMEM((subs, cells, LANES), jnp.float32),
            pltpu.VMEM((subs, rows, cells), jnp.float32),
            pltpu.VMEM((sub_count * subs, rows, cells), jnp.float32),
            pltpu.SemaphoreType.DMA((2, subs, halves)),
            pltpu.SemaphoreType.DMA((5,)),
            pltpu.SemaphoreType.DMA((STEPS, 2, chunks)),
            pltpu.SemaphoreType.DMA((STEPS, 2, chunks)),
            pltpu.SemaphoreType.DMA((sub_count - 1,)),
            pltpu.SemaphoreType.DMA((sub_count - 1,)),
        ],
        compiler_params=pltpu.CompilerParams(
            collective_id=0, has_side_effects=True, vmem_limit_bytes=40 * 1024 * 1024
        ),
        name="steps_and_planes",
    )(*(pltpu.with_memory_space_constraint(a, pltpu.HBM) for a in arrays))
    return pl.pallas_call(
        put_out,
        out_shape=tuple(jax.ShapeDtypeStruct(r.shape, r.dtype) for r in results),
        in_specs=[pl.BlockSpec(memory_space=pl.ANY)] * 2,
        out_specs=(pl.BlockSpec(memory_space=pl.ANY),) * 2,
        scratch_shapes=[pltpu.SemaphoreType.DMA((subs, 4)), pltpu.SemaphoreType.DMA],
        compiler_params=pltpu.CompilerParams(vmem_limit_bytes=1024 * 1024),
        name="put_out",
    )(*results)


def solution(mesh):
    sub_count, ring = mesh.shape["sub"], mesh.shape["gx"]

    def whole(value_field, *others):
        total_subs, total_rows, cells, third = value_field.shape
        dims = (
            total_subs // sub_count,
            total_rows // ring,
            cells,
            third // LANES,
            sub_count,
            ring,
            total_rows,
        )
        step = jax.shard_map(
            functools.partial(on_device, dims),
            mesh=mesh,
            in_specs=(
                P("sub", "gx", None, None),
                P("sub", "gx", None, None),
                P("sub", None, None),
                P("sub", None),
                P("sub", None),
                P(),
                P("sub"),
            ),
            out_specs=(P("sub", "gx", None, None), P("sub", "gx", None)),
            check_vma=False,
        )
        return step(value_field, *others)

    return whole
```

```python
import functools

import jax
import jax.numpy as jnp
from jax import lax
from jax.experimental import pallas as pl
from jax.experimental.pallas import tpu as pltpu
from jax.sharding import PartitionSpec as P

STEPS = 2
LANES = 128
PAD = 8
TS = 16
LINE = 4
LAG = 2
LEAD = 6
BLOCKS = 8


def pick(a, abs_a, b, abs_b):
    return jnp.where(abs_a <= abs_b, a, b)


def rank_of(sub):
    return sub + 1 - 2 * lax.rem(sub, 2)


def kernel(
    dims,
    value_hbm,
    speed_hbm,
    matrix_hbm,
    offset_hbm,
    bound_hbm,
    partner_hbm,
    dropped_hbm,
    final,
    shared_ref,
    first,
    second,
    speed,
    drift_matrix,
    drift_offset,
    control_bound,
    partner_table,
    dropped_dim,
    low_second,
    low_third,
    own,
    gathered,
    load_sem,
    scalar_sem,
    send_sem,
    recv_sem,
    plane_send,
    plane_recv,
    ready,
):
    subs, rows, cells, halves, sub_count, ring, total_rows = dims
    block = cells // BLOCKS
    chunks = subs * BLOCKS
    sub_at = lax.axis_index("sub")
    at = lax.axis_index("gx")
    right = lax.rem(at + 1, ring)
    left = lax.rem(at + ring - 1, ring)
    peers = [lax.rem(sub_at + k, sub_count) for k in range(1, sub_count)]

    spacing = (2.0 / total_rows, 2.0 / cells, 2.0 / (halves * LANES))
    time_step = min(spacing) / 15.0
    scale = tuple(time_step / (2.0 * h) for h in spacing)

    barrier = pltpu.get_barrier_semaphore()
    for target in (left, right):
        pl.semaphore_signal(barrier, inc=1, device_id={"gx": target}, device_id_type=pl.DeviceIdType.MESH)
    rank = rank_of(sub_at)
    for target in peers:

        @pl.when(rank_of(target) > rank)
        def _():
            pl.semaphore_signal(barrier, inc=1, device_id={"sub": target}, device_id_type=pl.DeviceIdType.MESH)

    def loads(source, held, spans, first_row, pad, kind):
        return [
            pltpu.make_async_copy(
                source.at[s, pl.ds(low, count), :, pl.ds(h * LANES, LANES)],
                held.at[s, pl.ds(first_row + low, count), h, pl.ds(pad, cells), :],
                load_sem.at[kind + k, s, h],
            )
            for k, (low, count) in enumerate(spans)
            for s in range(subs)
            for h in range(halves)
        ]

    rim_loads = loads(value_hbm, first, ((0, 2), (rows - 2, 2)), 2, PAD, 0)
    other_loads = loads(value_hbm, first, ((2, rows - 4),), 2, PAD, 2)
    other_loads += loads(speed_hbm, speed, ((0, rows),), 0, 0, 3)
    other_loads += [
        pltpu.make_async_copy(source, held, scalar_sem.at[k])
        for k, (source, held) in enumerate(
            (
                (matrix_hbm, drift_matrix),
                (offset_hbm, drift_offset),
                (bound_hbm, control_bound),
                (partner_hbm, partner_table),
                (dropped_hbm, dropped_dim),
            )
        )
    ]
    for copy in rim_loads + other_loads:
        copy.start()
    pl.semaphore_wait(barrier, 2 + rank)
    for target in peers:

        @pl.when(rank_of(target) < rank)
        def _():
            pl.semaphore_signal(ready, inc=1, device_id={"sub": target}, device_id_type=pl.DeviceIdType.MESH)


    def rim_copy(step, chunk, way):
        s = chunk // BLOCKS
        cells_sent = pl.ds(PAD + lax.rem(chunk, BLOCKS) * block, block)
        held = first if step == 0 else second
        return pltpu.make_async_remote_copy(
            src_ref=held.at[s, pl.ds(2 + (rows - 2) * (1 - way), 2), :, cells_sent, :],
            dst_ref=held.at[s, pl.ds((rows + 2) * way, 2), :, cells_sent, :],
            send_sem=send_sem.at[step, way, chunk],
            recv_sem=recv_sem.at[step, way, chunk],
            device_id={"gx": lax.rem(at + ring + 1 - 2 * way, ring)},
            device_id_type=pl.DeviceIdType.MESH,
        )

    for copy in rim_loads:
        copy.wait()

    @pl.loop(0, chunks)
    def _(chunk):
        for way in range(2):
            rim_copy(0, chunk, way).start()

    for copy in other_loads:
        copy.wait()

    def repeat_end(held, s, cell, start):
        for r in range(rows):
            for h in range(halves):
                held[s, r + 2, h, pl.ds(start, 2), :] = jnp.broadcast_to(
                    held[s, r + 2, h, pl.ds(cell, 1), :], (2, LANES)
                )

    first_end, last_end = (PAD, PAD - 2), (PAD + cells - 1, PAD + cells)

    @pl.loop(0, subs)
    def _(s):
        repeat_end(first, s, *first_end)
        repeat_end(first, s, *last_end)

    lane = lax.broadcasted_iota(jnp.int32, (TS, LANES), 1)
    at_start = lane == 0
    at_end = lane == LANES - 1
    low_third[...] = jnp.zeros_like(low_third)
    low_second[...] = jnp.full_like(low_second, jnp.inf)

    def coordinate(index, total):
        return -1.0 + (index.astype(jnp.float32) + 0.5) * (2.0 / total)

    def ahead(parts, edge):
        turned = [pltpu.roll(p, LANES - 1, 1) for p in parts]
        return [
            jnp.where(at_end, turned[h + 1] if h + 1 < halves else edge, turned[h])
            for h in range(halves)
        ]

    def behind(parts, edge):
        turned = [pltpu.roll(p, 1, 1) for p in parts]
        return [
            jnp.where(at_start, turned[h - 1] if h > 0 else edge, turned[h]) for h in range(halves)
        ]

    def cells_of(held, step, s, low_row, count, start):
        matrix = [[drift_matrix[d, s, e] * scale[d] for e in range(3)] for d in range(3)]
        offset = [drift_offset[s, d] * scale[d] for d in range(3)]
        bound = [control_bound[s, d] * scale[d] for d in range(3)]
        index = start + lax.broadcasted_iota(jnp.int32, (TS, LANES), 0)
        second_axis = coordinate(index, cells)
        drift_base = []
        for h in range(halves):
            third_axis = coordinate(lane + h * LANES, halves * LANES)
            drift_base.append(
                [matrix[d][1] * second_axis + matrix[d][2] * third_axis for d in range(3)]
            )
        lows = low_third[s, pl.ds(start, TS), :] if step == 1 else None

        def value(r, h, shift=0):
            return held[s, low_row + r + 2, h, pl.ds(PAD + start + shift, TS), :]

        middle = {r: [value(r, h) for h in range(halves)] for r in range(-2, count + 2)}
        along_first = {}
        for h in range(halves):
            slope = {r: middle[r + 1][h] - middle[r][h] for r in range(-2, count + 1)}
            curve = {r: slope[r] - slope[r - 1] for r in range(-1, count + 1)}
            size = {r: jnp.abs(curve[r]) for r in curve}
            for r in range(-1, count):
                face = pick(curve[r], size[r], curve[r + 1], size[r + 1])
                twice = slope[r] + slope[r]
                along_first[r, h, 0] = twice - face
                along_first[r + 1, h, 1] = -(twice + face)
        for r in range(count):
            row = low_row + r
            x0 = -1.0 + ((at * rows + row).astype(jnp.float32) + 0.5) * (2.0 / total_rows)
            center = middle[r]
            up = ahead(center, center[halves - 1])
            down = behind(center, center[0])
            plus = [up[h] - center[h] for h in range(halves)]
            minus = [down[h] - center[h] for h in range(halves)]
            curve = [plus[h] + minus[h] for h in range(halves)]
            curve_up = ahead(curve, 0.0)
            curve_down = behind(curve, 0.0)
            results = []
            for h in range(halves):
                sides = [(along_first[r, h, 0], along_first[r, h, 1])]
                a2, a1, b1, b2 = (value(r, h, k) for k in (-2, -1, 1, 2))
                p = b1 - center[h]
                m = a1 - center[h]
                c = p + m
                c_up = (b2 - b1) - p
                c_down = (a2 - a1) - m
                size, size_up, size_down = jnp.abs(c), jnp.abs(c_up), jnp.abs(c_down)
                sides.append(
                    (
                        (p + p) - pick(c, size, c_up, size_up),
                        (m + m) - pick(c_down, size_down, c, size),
                    )
                )
                c, c_up, c_down = curve[h], curve_up[h], curve_down[h]
                size, size_up, size_down = jnp.abs(c), jnp.abs(c_up), jnp.abs(c_down)
                sides.append(
                    (
                        (plus[h] + plus[h]) - pick(c, size, c_up, size_up),
                        (minus[h] + minus[h]) - pick(c_down, size_down, c, size),
                    )
                )
                drifting = None
                reaching = None
                for d, (x, y) in enumerate(sides):
                    drift = drift_base[h][d] + (offset[d] + matrix[d][0] * x0)
                    term = jnp.abs(drift) * jnp.where(drift >= 0.0, y, x)
                    reach = bound[d] * jnp.maximum(x, y)
                    drifting = term if drifting is None else drifting + term
                    reaching = reach if reaching is None else reaching + reach
                gain = drifting + speed[s, row, h, pl.ds(start, TS), :] * reaching
                result = center[h] + jnp.minimum(gain, 0.0)
                results.append(result)
                if step == 0:
                    second[s, row + 2, h, pl.ds(PAD + start, TS), :] = result
                else:
                    final[s, row, pl.ds(start, TS), pl.ds(h * LANES, LANES)] = result
                    low = result[:8]
                    for k in range(8, TS, 8):
                        low = jnp.minimum(low, result[k : k + 8])
                    low_second[s, row, h] = jnp.minimum(low_second[s, row, h], low)
            if step == 1:
                joint = results[0]
                for part in results[1:]:
                    joint = jnp.minimum(joint, part)
                least = jnp.min(joint, axis=1, keepdims=True)
                lows = jnp.where(lane == row, least, lows)
        if step == 1:
            low_third[s, pl.ds(start, TS), :] = lows

    def run(step, chunk, low_row, count):
        s = chunk // BLOCKS
        j = lax.rem(chunk, BLOCKS) * block

        @pl.loop(0, block // TS)
        def _(t):
            cells_of(
                second if step else first, step, s, low_row, count, pl.multiple_of(j + t * TS, TS)
            )

    def inner(step, chunk):
        run(step, chunk, 2, rows - 4)

    def side(step, chunk, way):
        rim_copy(step, chunk, way).wait_recv()
        run(step, chunk, (rows - 2) * way, 2)
        if step == 0:
            rim_copy(1, chunk, 1 - way).start()

    late = lax.rem(at, LINE) // (LINE // 2)
    early = 1 - late

    @pl.loop(0, LEAD)
    def _(chunk):
        inner(0, chunk)

    @pl.loop(0, chunks + LAG + 1)
    def _(i):
        @pl.when(i + LEAD < chunks)
        def _():
            inner(0, i + LEAD)

        @pl.when(i < chunks)
        def _():
            side(0, i, early)

        @pl.when((i >= LAG) & (i < chunks + LAG))
        def _():
            chunk = i - LAG
            s = chunk // BLOCKS
            side(0, chunk, late)

            @pl.when(lax.rem(chunk, BLOCKS) == 0)
            def _():
                repeat_end(second, s, *first_end)

            @pl.when(lax.rem(chunk, BLOCKS) == BLOCKS - 1)
            def _():
                repeat_end(second, s, *last_end)

        @pl.when(i > LAG)
        def _():
            inner(1, i - LAG - 1)

    def plane_copy(s, k):
        return pltpu.make_async_remote_copy(
            src_ref=own.at[s],
            dst_ref=gathered.at[sub_at * subs + s],
            send_sem=plane_send.at[s, k],
            recv_sem=plane_recv.at[s, k],
            device_id={"sub": peers[k]},
            device_id_type=pl.DeviceIdType.MESH,
        )

    @pl.when(rank < sub_count - 1)
    def _():
        pl.semaphore_wait(ready, sub_count - 1 - rank)

    @pl.loop(0, chunks + LAG)
    def _(i):
        @pl.when(i < chunks)
        def _():
            side(1, i, early)

        @pl.when(i >= LAG)
        def _():
            side(1, i - LAG, late)

        @pl.when((i >= LAG) & (lax.rem(i + BLOCKS - LAG, BLOCKS) == BLOCKS - 1))
        def _():
            s = (i - LAG) // BLOCKS
            over_third = jnp.transpose(low_third[s])[:rows]
            for h in range(halves):
                over_second = jnp.min(low_second[s, :, h], axis=1)
                plane = jnp.where(
                    dropped_dim[s] == 1, over_second, over_third[:, h * LANES : (h + 1) * LANES]
                )
                own[s, :, pl.ds(h * LANES, LANES)] = plane
                gathered[sub_at * subs + s, :, pl.ds(h * LANES, LANES)] = plane
            for k in range(len(peers)):
                plane_copy(s, k).start()

    @pl.loop(0, chunks)
    def _(chunk):
        for step in range(STEPS):
            for way in range(2):
                rim_copy(step, chunk, way).wait_send()

    for s in range(subs):
        for k in range(len(peers)):
            plane_copy(s, k).wait_recv()
    for s in range(subs):
        partner = partner_table[sub_at * subs + s]
        shared_ref[s] = jnp.maximum(own[s], gathered[partner])
    for s in range(subs):
        for k in range(len(peers)):
            plane_copy(s, k).wait_send()


def put_out(final, shared, final_out, shared_out, final_sem, shared_sem):
    subs, rows = final.shape[:2]
    pieces = final_sem.shape[1]
    count = rows // pieces
    copies = [pltpu.make_async_copy(shared, shared_out, shared_sem)]
    for s in range(subs):
        for k in range(pieces):
            at = (s, pl.ds(k * count, count))
            copies.append(pltpu.make_async_copy(final.at[at], final_out.at[at], final_sem.at[s, k]))
    for copy in copies:
        copy.start()
    for copy in copies:
        copy.wait()


def on_device(dims, value_field, speed_field, drift_matrix, *others):
    subs, rows, cells, halves, sub_count, ring, total_rows = dims
    chunks = subs * BLOCKS
    in_vmem = pl.BlockSpec(memory_space=pltpu.VMEM)
    held = pltpu.VMEM((subs, rows + 4, halves, cells + 3 * PAD, LANES), jnp.float32)
    whole = pltpu.VMEM((subs, rows, halves, cells + PAD, LANES), jnp.float32)
    arrays = (value_field, speed_field, jnp.transpose(drift_matrix, (1, 0, 2)), *others)
    results = pl.pallas_call(
        functools.partial(kernel, dims),
        out_shape=(
            jax.ShapeDtypeStruct((subs, rows, cells, halves * LANES), jnp.float32),
            jax.ShapeDtypeStruct((subs, rows, cells), jnp.float32),
        ),
        in_specs=[pl.BlockSpec(memory_space=pltpu.HBM)] * 7,
        out_specs=(in_vmem, in_vmem),
        scratch_shapes=[
            held,
            held,
            whole,
            pltpu.SMEM((3, subs, 3), jnp.float32),
            pltpu.SMEM((subs, 3), jnp.float32),
            pltpu.SMEM((subs, 3), jnp.float32),
            pltpu.SMEM((sub_count * subs,), jnp.int32),
            pltpu.SMEM((subs,), jnp.int32),
            pltpu.VMEM((subs, rows, halves, 8, LANES), jnp.float32),
            pltpu.VMEM((subs, cells, LANES), jnp.float32),
            pltpu.VMEM((subs, rows, cells), jnp.float32),
            pltpu.VMEM((sub_count * subs, rows, cells), jnp.float32),
            pltpu.SemaphoreType.DMA((4, subs, halves)),
            pltpu.SemaphoreType.DMA((5,)),
            pltpu.SemaphoreType.DMA((STEPS, 2, chunks)),
            pltpu.SemaphoreType.DMA((STEPS, 2, chunks)),
            pltpu.SemaphoreType.DMA((subs, sub_count - 1)),
            pltpu.SemaphoreType.DMA((subs, sub_count - 1)),
            pltpu.SemaphoreType.REGULAR,
        ],
        compiler_params=pltpu.CompilerParams(
            collective_id=0, has_side_effects=True, vmem_limit_bytes=40 * 1024 * 1024
        ),
        name="steps_and_planes",
    )(*(pltpu.with_memory_space_constraint(a, pltpu.HBM) for a in arrays))
    return pl.pallas_call(
        put_out,
        out_shape=tuple(jax.ShapeDtypeStruct(r.shape, r.dtype) for r in results),
        in_specs=[pl.BlockSpec(memory_space=pl.ANY)] * 2,
        out_specs=(pl.BlockSpec(memory_space=pl.ANY),) * 2,
        scratch_shapes=[pltpu.SemaphoreType.DMA((subs, 4)), pltpu.SemaphoreType.DMA],
        compiler_params=pltpu.CompilerParams(vmem_limit_bytes=1024 * 1024),
        name="put_out",
    )(*results)


def solution(mesh):
    sub_count, ring = mesh.shape["sub"], mesh.shape["gx"]

    def whole(value_field, *others):
        total_subs, total_rows, cells, third = value_field.shape
        dims = (
            total_subs // sub_count,
            total_rows // ring,
            cells,
            third // LANES,
            sub_count,
            ring,
            total_rows,
        )
        step = jax.shard_map(
            functools.partial(on_device, dims),
            mesh=mesh,
            in_specs=(
                P("sub", "gx", None, None),
                P("sub", "gx", None, None),
                P("sub", None, None),
                P("sub", None),
                P("sub", None),
                P(),
                P("sub"),
            ),
            out_specs=(P("sub", "gx", None, None), P("sub", "gx", None)),
            check_vma=False,
        )
        return step(value_field, *others)

    return whole
```

```python
import functools

import jax
import jax.numpy as jnp
from jax import lax
from jax.experimental import pallas as pl
from jax.experimental.pallas import tpu as pltpu
from jax.sharding import PartitionSpec as P

STEPS = 2
LANES = 128
PAD = 8
TS = 16
LINE = 4
LAG = 2
LEAD = 6
BLOCKS = 8


def pick(a, abs_a, b, abs_b):
    return jnp.where(abs_a <= abs_b, a, b)


def rank_of(sub):
    return sub + 1 - 2 * lax.rem(sub, 2)


def kernel(
    dims,
    value_hbm,
    speed_hbm,
    matrix_hbm,
    offset_hbm,
    bound_hbm,
    partner_hbm,
    dropped_hbm,
    final,
    shared_ref,
    first,
    second,
    speed,
    drift_matrix,
    drift_offset,
    control_bound,
    partner_table,
    dropped_dim,
    low_second,
    low_third,
    own,
    gathered,
    load_sem,
    scalar_sem,
    send_sem,
    recv_sem,
    plane_send,
    plane_recv,
    ready,
):
    subs, rows, cells, halves, sub_count, ring, total_rows = dims
    block = cells // BLOCKS
    chunks = subs * BLOCKS
    sub_at = lax.axis_index("sub")
    at = lax.axis_index("gx")
    right = lax.rem(at + 1, ring)
    left = lax.rem(at + ring - 1, ring)
    peers = [lax.rem(sub_at + k, sub_count) for k in range(1, sub_count)]

    spacing = (2.0 / total_rows, 2.0 / cells, 2.0 / (halves * LANES))
    time_step = min(spacing) / 15.0
    scale = tuple(time_step / (2.0 * h) for h in spacing)

    barrier = pltpu.get_barrier_semaphore()
    for target in (left, right):
        pl.semaphore_signal(barrier, inc=1, device_id={"gx": target}, device_id_type=pl.DeviceIdType.MESH)
    rank = rank_of(sub_at)
    for target in peers:

        @pl.when(rank_of(target) > rank)
        def _():
            pl.semaphore_signal(barrier, inc=1, device_id={"sub": target}, device_id_type=pl.DeviceIdType.MESH)

    def loads(source, held, spans, first_row, pad, kind):
        return [
            pltpu.make_async_copy(
                source.at[:, pl.ds(low, count), :, pl.ds(h * LANES, LANES)],
                held.at[:, pl.ds(first_row + low, count), h, pl.ds(pad, cells), :],
                load_sem.at[kind + k, h],
            )
            for k, (low, count) in enumerate(spans)
            for h in range(halves)
        ]

    rim_loads = loads(value_hbm, first, ((0, 2), (rows - 2, 2)), 2, PAD, 0)
    other_loads = loads(value_hbm, first, ((2, rows - 4),), 2, PAD, 2)
    other_loads += loads(speed_hbm, speed, ((0, rows),), 0, 0, 3)
    other_loads += [
        pltpu.make_async_copy(source, held, scalar_sem.at[k])
        for k, (source, held) in enumerate(
            (
                (matrix_hbm, drift_matrix),
                (offset_hbm, drift_offset),
                (bound_hbm, control_bound),
                (partner_hbm, partner_table),
                (dropped_hbm, dropped_dim),
            )
        )
    ]
    for copy in rim_loads + other_loads:
        copy.start()
    pl.semaphore_wait(barrier, 2 + rank)
    for target in peers:

        @pl.when(rank_of(target) < rank)
        def _():
            pl.semaphore_signal(ready, inc=1, device_id={"sub": target}, device_id_type=pl.DeviceIdType.MESH)


    def rim_copy(step, chunk, way):
        s = chunk // BLOCKS
        cells_sent = pl.ds(PAD + lax.rem(chunk, BLOCKS) * block, block)
        held = first if step == 0 else second
        return pltpu.make_async_remote_copy(
            src_ref=held.at[s, pl.ds(2 + (rows - 2) * (1 - way), 2), :, cells_sent, :],
            dst_ref=held.at[s, pl.ds((rows + 2) * way, 2), :, cells_sent, :],
            send_sem=send_sem.at[step, way],
            recv_sem=recv_sem.at[step, way, chunk],
            device_id={"gx": lax.rem(at + ring + 1 - 2 * way, ring)},
            device_id_type=pl.DeviceIdType.MESH,
        )

    for copy in rim_loads:
        copy.wait()

    @pl.loop(0, chunks)
    def _(chunk):
        for way in range(2):
            rim_copy(0, chunk, way).start()

    for copy in other_loads:
        copy.wait()

    def repeat_end(held, s, cell, start):
        for r in range(rows):
            for h in range(halves):
                held[s, r + 2, h, pl.ds(start, 2), :] = jnp.broadcast_to(
                    held[s, r + 2, h, pl.ds(cell, 1), :], (2, LANES)
                )

    first_end, last_end = (PAD, PAD - 2), (PAD + cells - 1, PAD + cells)

    @pl.loop(0, subs)
    def _(s):
        repeat_end(first, s, *first_end)
        repeat_end(first, s, *last_end)

    low_third[...] = jnp.zeros_like(low_third)
    low_second[...] = jnp.full_like(low_second, jnp.inf)

    def coordinate(index, total):
        return -1.0 + (index.astype(jnp.float32) + 0.5) * (2.0 / total)

    def ahead(parts, edge):
        at_end = lax.broadcasted_iota(jnp.int32, parts[0].shape, 1) == LANES - 1
        turned = [pltpu.roll(p, LANES - 1, 1) for p in parts]
        return [
            jnp.where(at_end, turned[h + 1] if h + 1 < halves else edge, turned[h])
            for h in range(halves)
        ]

    def behind(parts, edge):
        at_start = lax.broadcasted_iota(jnp.int32, parts[0].shape, 1) == 0
        turned = [pltpu.roll(p, 1, 1) for p in parts]
        return [
            jnp.where(at_start, turned[h - 1] if h > 0 else edge, turned[h]) for h in range(halves)
        ]

    def cells_of(held, step, s, low_row, count, start, size_of_block):
        matrix = [[drift_matrix[d, s, e] * scale[d] for e in range(3)] for d in range(3)]
        offset = [drift_offset[s, d] * scale[d] for d in range(3)]
        bound = [control_bound[s, d] * scale[d] for d in range(3)]
        lane = lax.broadcasted_iota(jnp.int32, (size_of_block, LANES), 1)
        index = start + lax.broadcasted_iota(jnp.int32, (size_of_block, LANES), 0)
        second_axis = coordinate(index, cells)
        drift_base = []
        for h in range(halves):
            third_axis = coordinate(lane + h * LANES, halves * LANES)
            drift_base.append(
                [matrix[d][1] * second_axis + matrix[d][2] * third_axis for d in range(3)]
            )
        lows = low_third[s, pl.ds(start, size_of_block), :] if step == 1 else None

        def value(r, h, shift=0):
            return held[s, low_row + r + 2, h, pl.ds(PAD + start + shift, size_of_block), :]

        middle = {r: [value(r, h) for h in range(halves)] for r in range(-2, count + 2)}
        along_first = {}
        for h in range(halves):
            slope = {r: middle[r + 1][h] - middle[r][h] for r in range(-2, count + 1)}
            curve = {r: slope[r] - slope[r - 1] for r in range(-1, count + 1)}
            size = {r: jnp.abs(curve[r]) for r in curve}
            for r in range(-1, count):
                face = pick(curve[r], size[r], curve[r + 1], size[r + 1])
                twice = slope[r] + slope[r]
                along_first[r, h, 0] = twice - face
                along_first[r + 1, h, 1] = -(twice + face)
        for r in range(count):
            row = low_row + r
            x0 = -1.0 + ((at * rows + row).astype(jnp.float32) + 0.5) * (2.0 / total_rows)
            center = middle[r]
            up = ahead(center, center[halves - 1])
            down = behind(center, center[0])
            plus = [up[h] - center[h] for h in range(halves)]
            minus = [down[h] - center[h] for h in range(halves)]
            curve = [plus[h] + minus[h] for h in range(halves)]
            curve_up = ahead(curve, 0.0)
            curve_down = behind(curve, 0.0)
            results = []
            for h in range(halves):
                sides = [(along_first[r, h, 0], along_first[r, h, 1])]
                a2, a1, b1, b2 = (value(r, h, k) for k in (-2, -1, 1, 2))
                p = b1 - center[h]
                m = a1 - center[h]
                c = p + m
                c_up = (b2 - b1) - p
                c_down = (a2 - a1) - m
                size, size_up, size_down = jnp.abs(c), jnp.abs(c_up), jnp.abs(c_down)
                sides.append(
                    (
                        (p + p) - pick(c, size, c_up, size_up),
                        (m + m) - pick(c_down, size_down, c, size),
                    )
                )
                c, c_up, c_down = curve[h], curve_up[h], curve_down[h]
                size, size_up, size_down = jnp.abs(c), jnp.abs(c_up), jnp.abs(c_down)
                sides.append(
                    (
                        (plus[h] + plus[h]) - pick(c, size, c_up, size_up),
                        (minus[h] + minus[h]) - pick(c_down, size_down, c, size),
                    )
                )
                drifting = None
                reaching = None
                for d, (x, y) in enumerate(sides):
                    drift = drift_base[h][d] + (offset[d] + matrix[d][0] * x0)
                    term = jnp.abs(drift) * jnp.where(drift >= 0.0, y, x)
                    reach = bound[d] * jnp.maximum(x, y)
                    drifting = term if drifting is None else drifting + term
                    reaching = reach if reaching is None else reaching + reach
                gain = drifting + speed[s, row, h, pl.ds(start, size_of_block), :] * reaching
                result = center[h] + jnp.minimum(gain, 0.0)
                results.append(result)
                if step == 0:
                    second[s, row + 2, h, pl.ds(PAD + start, size_of_block), :] = result
                else:
                    final[s, row, pl.ds(start, size_of_block), pl.ds(h * LANES, LANES)] = result
                    low = result[:8]
                    for k in range(8, size_of_block, 8):
                        low = jnp.minimum(low, result[k : k + 8])
                    low_second[s, row, h] = jnp.minimum(low_second[s, row, h], low)
            if step == 1:
                joint = results[0]
                for part in results[1:]:
                    joint = jnp.minimum(joint, part)
                least = jnp.min(joint, axis=1, keepdims=True)
                lows = jnp.where(lane == row, least, lows)
        if step == 1:
            low_third[s, pl.ds(start, size_of_block), :] = lows

    def run(step, chunk, low_row, count, size_of_block):
        s = chunk // BLOCKS
        j = lax.rem(chunk, BLOCKS) * block

        @pl.loop(0, block // size_of_block)
        def _(t):
            start = pl.multiple_of(j + t * size_of_block, size_of_block)
            cells_of(second if step else first, step, s, low_row, count, start, size_of_block)

    def inner(step, chunk):
        run(step, chunk, 2, rows - 4, TS)

    def side(step, chunk, way):
        rim_copy(step, chunk, way).wait_recv()
        run(step, chunk, (rows - 2) * way, 2, 2 * TS)
        if step == 0:
            rim_copy(1, chunk, 1 - way).start()

    late = lax.rem(at, LINE) // (LINE // 2)
    early = 1 - late

    @pl.loop(0, LEAD)
    def _(chunk):
        inner(0, chunk)

    @pl.loop(0, chunks + LAG + 1)
    def _(i):
        @pl.when(i + LEAD < chunks)
        def _():
            inner(0, i + LEAD)

        @pl.when(i < chunks)
        def _():
            side(0, i, early)

        @pl.when((i >= LAG) & (i < chunks + LAG))
        def _():
            chunk = i - LAG
            s = chunk // BLOCKS
            side(0, chunk, late)

            @pl.when(lax.rem(chunk, BLOCKS) == 0)
            def _():
                repeat_end(second, s, *first_end)

            @pl.when(lax.rem(chunk, BLOCKS) == BLOCKS - 1)
            def _():
                repeat_end(second, s, *last_end)

        @pl.when(i > LAG)
        def _():
            inner(1, i - LAG - 1)

    def plane_copy(s, k):
        return pltpu.make_async_remote_copy(
            src_ref=own.at[s],
            dst_ref=gathered.at[sub_at * subs + s],
            send_sem=plane_send.at[s, k],
            recv_sem=plane_recv.at[s, k],
            device_id={"sub": peers[k]},
            device_id_type=pl.DeviceIdType.MESH,
        )

    @pl.when(rank < sub_count - 1)
    def _():
        pl.semaphore_wait(ready, sub_count - 1 - rank)

    @pl.loop(0, chunks + LAG)
    def _(i):
        @pl.when(i < chunks)
        def _():
            side(1, i, early)

        @pl.when(i >= LAG)
        def _():
            side(1, i - LAG, late)

        @pl.when((i >= LAG) & (lax.rem(i + BLOCKS - LAG, BLOCKS) == BLOCKS - 1))
        def _():
            s = (i - LAG) // BLOCKS
            over_third = jnp.transpose(low_third[s])[:rows]
            for h in range(halves):
                over_second = jnp.min(low_second[s, :, h], axis=1)
                plane = jnp.where(
                    dropped_dim[s] == 1, over_second, over_third[:, h * LANES : (h + 1) * LANES]
                )
                own[s, :, pl.ds(h * LANES, LANES)] = plane
                gathered[sub_at * subs + s, :, pl.ds(h * LANES, LANES)] = plane
            for k in range(len(peers)):
                plane_copy(s, k).start()

    for step in range(STEPS):
        for way in range(2):
            every = (first if step == 0 else second).at[:, pl.ds(2, 2), :, pl.ds(PAD, cells), :]
            pltpu.make_async_remote_copy(
                src_ref=every,
                dst_ref=every,
                send_sem=send_sem.at[step, way],
                recv_sem=recv_sem.at[step, way, 0],
                device_id={"gx": right},
                device_id_type=pl.DeviceIdType.MESH,
            ).wait_send()

    for s in range(subs):
        for k in range(len(peers)):
            plane_copy(s, k).wait_recv()
    for s in range(subs):
        partner = partner_table[sub_at * subs + s]
        shared_ref[s] = jnp.maximum(own[s], gathered[partner])
    for s in range(subs):
        for k in range(len(peers)):
            plane_copy(s, k).wait_send()


def put_out(final, shared, final_out, shared_out, final_sem, shared_sem):
    subs, rows = final.shape[:2]
    pieces = final_sem.shape[1]
    count = rows // pieces
    copies = [pltpu.make_async_copy(shared, shared_out, shared_sem)]
    for s in range(subs):
        for k in range(pieces):
            at = (s, pl.ds(k * count, count))
            copies.append(pltpu.make_async_copy(final.at[at], final_out.at[at], final_sem.at[s, k]))
    for copy in copies:
        copy.start()
    for copy in copies:
        copy.wait()


def on_device(dims, value_field, speed_field, drift_matrix, *others):
    subs, rows, cells, halves, sub_count, ring, total_rows = dims
    chunks = subs * BLOCKS
    in_vmem = pl.BlockSpec(memory_space=pltpu.VMEM)
    held = pltpu.VMEM((subs, rows + 4, halves, cells + 3 * PAD, LANES), jnp.float32)
    whole = pltpu.VMEM((subs, rows, halves, cells + PAD, LANES), jnp.float32)
    arrays = (value_field, speed_field, jnp.transpose(drift_matrix, (1, 0, 2)), *others)
    results = pl.pallas_call(
        functools.partial(kernel, dims),
        out_shape=(
            jax.ShapeDtypeStruct((subs, rows, cells, halves * LANES), jnp.float32),
            jax.ShapeDtypeStruct((subs, rows, cells), jnp.float32),
        ),
        in_specs=[pl.BlockSpec(memory_space=pltpu.HBM)] * 7,
        out_specs=(in_vmem, in_vmem),
        scratch_shapes=[
            held,
            held,
            whole,
            pltpu.SMEM((3, subs, 3), jnp.float32),
            pltpu.SMEM((subs, 3), jnp.float32),
            pltpu.SMEM((subs, 3), jnp.float32),
            pltpu.SMEM((sub_count * subs,), jnp.int32),
            pltpu.SMEM((subs,), jnp.int32),
            pltpu.VMEM((subs, rows, halves, 8, LANES), jnp.float32),
            pltpu.VMEM((subs, cells, LANES), jnp.float32),
            pltpu.VMEM((subs, rows, cells), jnp.float32),
            pltpu.VMEM((sub_count * subs, rows, cells), jnp.float32),
            pltpu.SemaphoreType.DMA((4, halves)),
            pltpu.SemaphoreType.DMA((5,)),
            pltpu.SemaphoreType.DMA((STEPS, 2)),
            pltpu.SemaphoreType.DMA((STEPS, 2, chunks)),
            pltpu.SemaphoreType.DMA((subs, sub_count - 1)),
            pltpu.SemaphoreType.DMA((subs, sub_count - 1)),
            pltpu.SemaphoreType.REGULAR,
        ],
        compiler_params=pltpu.CompilerParams(
            collective_id=0, has_side_effects=True, vmem_limit_bytes=40 * 1024 * 1024
        ),
        name="steps_and_planes",
    )(*(pltpu.with_memory_space_constraint(a, pltpu.HBM) for a in arrays))
    return pl.pallas_call(
        put_out,
        out_shape=tuple(jax.ShapeDtypeStruct(r.shape, r.dtype) for r in results),
        in_specs=[pl.BlockSpec(memory_space=pl.ANY)] * 2,
        out_specs=(pl.BlockSpec(memory_space=pl.ANY),) * 2,
        scratch_shapes=[pltpu.SemaphoreType.DMA((subs, 4)), pltpu.SemaphoreType.DMA],
        compiler_params=pltpu.CompilerParams(vmem_limit_bytes=1024 * 1024),
        name="put_out",
    )(*results)


def solution(mesh):
    sub_count, ring = mesh.shape["sub"], mesh.shape["gx"]

    def whole(value_field, *others):
        total_subs, total_rows, cells, third = value_field.shape
        dims = (
            total_subs // sub_count,
            total_rows // ring,
            cells,
            third // LANES,
            sub_count,
            ring,
            total_rows,
        )
        step = jax.shard_map(
            functools.partial(on_device, dims),
            mesh=mesh,
            in_specs=(
                P("sub", "gx", None, None),
                P("sub", "gx", None, None),
                P("sub", None, None),
                P("sub", None),
                P("sub", None),
                P(),
                P("sub"),
            ),
            out_specs=(P("sub", "gx", None, None), P("sub", "gx", None)),
            check_vma=False,
        )
        return step(value_field, *others)

    return whole
```

```python
import functools

import jax
import jax.numpy as jnp
from jax import lax
from jax.experimental import pallas as pl
from jax.experimental.pallas import tpu as pltpu
from jax.sharding import PartitionSpec as P

STEPS = 2
LANES = 128
PAD = 8
TS = 16
LINE = 4
LAG = 1
LEAD = 6
BLOCKS = 8


def pick(a, abs_a, b, abs_b):
    return jnp.where(abs_a <= abs_b, a, b)


def rank_of(sub):
    return sub + 1 - 2 * lax.rem(sub, 2)


def kernel(
    dims,
    value_hbm,
    speed_hbm,
    matrix_hbm,
    offset_hbm,
    bound_hbm,
    partner_hbm,
    dropped_hbm,
    final,
    shared_ref,
    first,
    second,
    speed,
    drift_matrix,
    drift_offset,
    control_bound,
    partner_table,
    dropped_dim,
    low_second,
    low_third,
    own,
    gathered,
    load_sem,
    scalar_sem,
    send_sem,
    recv_sem,
    plane_send,
    plane_recv,
    ready,
):
    subs, rows, cells, halves, sub_count, ring, total_rows = dims
    block = cells // BLOCKS
    chunks = subs * BLOCKS
    sub_at = lax.axis_index("sub")
    at = lax.axis_index("gx")
    right = lax.rem(at + 1, ring)
    left = lax.rem(at + ring - 1, ring)
    peers = [lax.rem(sub_at + k, sub_count) for k in range(1, sub_count)]

    spacing = (2.0 / total_rows, 2.0 / cells, 2.0 / (halves * LANES))
    time_step = min(spacing) / 15.0
    scale = tuple(time_step / (2.0 * h) for h in spacing)

    barrier = pltpu.get_barrier_semaphore()
    for target in (left, right):
        pl.semaphore_signal(barrier, inc=1, device_id={"gx": target}, device_id_type=pl.DeviceIdType.MESH)
    rank = rank_of(sub_at)
    for target in peers:

        @pl.when(rank_of(target) > rank)
        def _():
            pl.semaphore_signal(barrier, inc=1, device_id={"sub": target}, device_id_type=pl.DeviceIdType.MESH)

    def loads(source, held, spans, first_row, pad, kind):
        return [
            pltpu.make_async_copy(
                source.at[:, pl.ds(low, count), :, pl.ds(h * LANES, LANES)],
                held.at[:, pl.ds(first_row + low, count), h, pl.ds(pad, cells), :],
                load_sem.at[kind + k, h],
            )
            for k, (low, count) in enumerate(spans)
            for h in range(halves)
        ]

    rim_loads = loads(value_hbm, first, ((0, 2), (rows - 2, 2)), 2, PAD, 0)
    other_loads = loads(value_hbm, first, ((2, rows - 4),), 2, PAD, 2)
    other_loads += loads(speed_hbm, speed, ((0, rows),), 0, 0, 3)
    other_loads += [
        pltpu.make_async_copy(source, held, scalar_sem.at[k])
        for k, (source, held) in enumerate(
            (
                (matrix_hbm, drift_matrix),
                (offset_hbm, drift_offset),
                (bound_hbm, control_bound),
                (partner_hbm, partner_table),
                (dropped_hbm, dropped_dim),
            )
        )
    ]
    for copy in rim_loads + other_loads:
        copy.start()
    pl.semaphore_wait(barrier, 2 + rank)
    for target in peers:

        @pl.when(rank_of(target) < rank)
        def _():
            pl.semaphore_signal(ready, inc=1, device_id={"sub": target}, device_id_type=pl.DeviceIdType.MESH)


    def rim_copy(step, chunk, way):
        s = chunk // BLOCKS
        cells_sent = pl.ds(PAD + lax.rem(chunk, BLOCKS) * block, block)
        held = first if step == 0 else second
        return pltpu.make_async_remote_copy(
            src_ref=held.at[s, pl.ds(2 + (rows - 2) * (1 - way), 2), :, cells_sent, :],
            dst_ref=held.at[s, pl.ds((rows + 2) * way, 2), :, cells_sent, :],
            send_sem=send_sem.at[step, way],
            recv_sem=recv_sem.at[step, way, chunk],
            device_id={"gx": lax.rem(at + ring + 1 - 2 * way, ring)},
            device_id_type=pl.DeviceIdType.MESH,
        )

    for copy in rim_loads:
        copy.wait()

    @pl.loop(0, chunks)
    def _(chunk):
        for way in range(2):
            rim_copy(0, chunk, way).start()

    for copy in other_loads:
        copy.wait()

    def repeat_end(held, s, cell, start):
        for r in range(rows):
            for h in range(halves):
                held[s, r + 2, h, pl.ds(start, 2), :] = jnp.broadcast_to(
                    held[s, r + 2, h, pl.ds(cell, 1), :], (2, LANES)
                )

    first_end, last_end = (PAD, PAD - 2), (PAD + cells - 1, PAD + cells)

    @pl.loop(0, subs)
    def _(s):
        repeat_end(first, s, *first_end)
        repeat_end(first, s, *last_end)

    low_third[...] = jnp.zeros_like(low_third)
    low_second[...] = jnp.full_like(low_second, jnp.inf)

    def coordinate(index, total):
        return -1.0 + (index.astype(jnp.float32) + 0.5) * (2.0 / total)

    def ahead(parts, edge):
        at_end = lax.broadcasted_iota(jnp.int32, parts[0].shape, 1) == LANES - 1
        turned = [pltpu.roll(p, LANES - 1, 1) for p in parts]
        return [
            jnp.where(at_end, turned[h + 1] if h + 1 < halves else edge, turned[h])
            for h in range(halves)
        ]

    def behind(parts, edge):
        at_start = lax.broadcasted_iota(jnp.int32, parts[0].shape, 1) == 0
        turned = [pltpu.roll(p, 1, 1) for p in parts]
        return [
            jnp.where(at_start, turned[h - 1] if h > 0 else edge, turned[h]) for h in range(halves)
        ]

    def cells_of(held, step, s, low_row, count, start, size_of_block):
        matrix = [[drift_matrix[d, s, e] * scale[d] for e in range(3)] for d in range(3)]
        offset = [drift_offset[s, d] * scale[d] for d in range(3)]
        bound = [control_bound[s, d] * scale[d] for d in range(3)]
        lane = lax.broadcasted_iota(jnp.int32, (size_of_block, LANES), 1)
        index = start + lax.broadcasted_iota(jnp.int32, (size_of_block, LANES), 0)
        second_axis = coordinate(index, cells)
        drift_base = []
        for h in range(halves):
            third_axis = coordinate(lane + h * LANES, halves * LANES)
            drift_base.append(
                [matrix[d][1] * second_axis + matrix[d][2] * third_axis for d in range(3)]
            )
        lows = low_third[s, pl.ds(start, size_of_block), :] if step == 1 else None

        def value(r, h, shift=0):
            return held[s, low_row + r + 2, h, pl.ds(PAD + start + shift, size_of_block), :]

        middle = {r: [value(r, h) for h in range(halves)] for r in range(-2, count + 2)}
        along_first = {}
        for h in range(halves):
            slope = {r: middle[r + 1][h] - middle[r][h] for r in range(-2, count + 1)}
            curve = {r: slope[r] - slope[r - 1] for r in range(-1, count + 1)}
            size = {r: jnp.abs(curve[r]) for r in curve}
            for r in range(-1, count):
                face = pick(curve[r], size[r], curve[r + 1], size[r + 1])
                twice = slope[r] + slope[r]
                along_first[r, h, 0] = twice - face
                along_first[r + 1, h, 1] = -(twice + face)
        for r in range(count):
            row = low_row + r
            x0 = -1.0 + ((at * rows + row).astype(jnp.float32) + 0.5) * (2.0 / total_rows)
            center = middle[r]
            up = ahead(center, center[halves - 1])
            down = behind(center, center[0])
            plus = [up[h] - center[h] for h in range(halves)]
            minus = [down[h] - center[h] for h in range(halves)]
            curve = [plus[h] + minus[h] for h in range(halves)]
            curve_up = ahead(curve, 0.0)
            curve_down = behind(curve, 0.0)
            results = []
            for h in range(halves):
                sides = [(along_first[r, h, 0], along_first[r, h, 1])]
                a2, a1, b1, b2 = (value(r, h, k) for k in (-2, -1, 1, 2))
                p = b1 - center[h]
                m = a1 - center[h]
                c = p + m
                c_up = (b2 - b1) - p
                c_down = (a2 - a1) - m
                size, size_up, size_down = jnp.abs(c), jnp.abs(c_up), jnp.abs(c_down)
                sides.append(
                    (
                        (p + p) - pick(c, size, c_up, size_up),
                        (m + m) - pick(c_down, size_down, c, size),
                    )
                )
                c, c_up, c_down = curve[h], curve_up[h], curve_down[h]
                size, size_up, size_down = jnp.abs(c), jnp.abs(c_up), jnp.abs(c_down)
                sides.append(
                    (
                        (plus[h] + plus[h]) - pick(c, size, c_up, size_up),
                        (minus[h] + minus[h]) - pick(c_down, size_down, c, size),
                    )
                )
                drifting = None
                reaching = None
                for d, (x, y) in enumerate(sides):
                    drift = drift_base[h][d] + (offset[d] + matrix[d][0] * x0)
                    term = jnp.abs(drift) * jnp.where(drift >= 0.0, y, x)
                    reach = bound[d] * jnp.maximum(x, y)
                    drifting = term if drifting is None else drifting + term
                    reaching = reach if reaching is None else reaching + reach
                gain = drifting + speed[s, row, h, pl.ds(start, size_of_block), :] * reaching
                result = center[h] + jnp.minimum(gain, 0.0)
                results.append(result)
                if step == 0:
                    second[s, row + 2, h, pl.ds(PAD + start, size_of_block), :] = result
                else:
                    final[s, row, pl.ds(start, size_of_block), pl.ds(h * LANES, LANES)] = result
                    low = result[:8]
                    for k in range(8, size_of_block, 8):
                        low = jnp.minimum(low, result[k : k + 8])
                    low_second[s, row, h] = jnp.minimum(low_second[s, row, h], low)
            if step == 1:
                joint = results[0]
                for part in results[1:]:
                    joint = jnp.minimum(joint, part)
                least = jnp.min(joint, axis=1, keepdims=True)
                lows = jnp.where(lane == row, least, lows)
        if step == 1:
            low_third[s, pl.ds(start, size_of_block), :] = lows

    def run(step, chunk, low_row, count, size_of_block):
        s = chunk // BLOCKS
        j = lax.rem(chunk, BLOCKS) * block

        @pl.loop(0, block // size_of_block)
        def _(t):
            start = pl.multiple_of(j + t * size_of_block, size_of_block)
            cells_of(second if step else first, step, s, low_row, count, start, size_of_block)

    def inner(step, chunk):
        run(step, chunk, 2, rows - 4, TS)

    def side(step, chunk, way):
        rim_copy(step, chunk, way).wait_recv()
        run(step, chunk, (rows - 2) * way, 2, 2 * TS)
        if step == 0:
            rim_copy(1, chunk, 1 - way).start()

    late = lax.rem(at, LINE) // (LINE // 2)
    early = 1 - late

    @pl.loop(0, LEAD)
    def _(chunk):
        inner(0, chunk)

    @pl.loop(0, chunks + LAG + 1)
    def _(i):
        @pl.when(i + LEAD < chunks)
        def _():
            inner(0, i + LEAD)

        @pl.when(i < chunks)
        def _():
            side(0, i, early)

        @pl.when((i >= LAG) & (i < chunks + LAG))
        def _():
            chunk = i - LAG
            s = chunk // BLOCKS
            side(0, chunk, late)

            @pl.when(lax.rem(chunk, BLOCKS) == 0)
            def _():
                repeat_end(second, s, *first_end)

            @pl.when(lax.rem(chunk, BLOCKS) == BLOCKS - 1)
            def _():
                repeat_end(second, s, *last_end)

        @pl.when(i > LAG)
        def _():
            inner(1, i - LAG - 1)

    def plane_copy(s, k):
        return pltpu.make_async_remote_copy(
            src_ref=own.at[s],
            dst_ref=gathered.at[sub_at * subs + s],
            send_sem=plane_send.at[s, k],
            recv_sem=plane_recv.at[s, k],
            device_id={"sub": peers[k]},
            device_id_type=pl.DeviceIdType.MESH,
        )

    @pl.when(rank < sub_count - 1)
    def _():
        pl.semaphore_wait(ready, sub_count - 1 - rank)

    @pl.loop(0, chunks + LAG)
    def _(i):
        @pl.when(i < chunks)
        def _():
            side(1, i, early)

        @pl.when(i >= LAG)
        def _():
            side(1, i - LAG, late)

        @pl.when((i >= LAG) & (lax.rem(i + BLOCKS - LAG, BLOCKS) == BLOCKS - 1))
        def _():
            s = (i - LAG) // BLOCKS
            over_third = jnp.transpose(low_third[s])[:rows]
            for h in range(halves):
                over_second = jnp.min(low_second[s, :, h], axis=1)
                plane = jnp.where(
                    dropped_dim[s] == 1, over_second, over_third[:, h * LANES : (h + 1) * LANES]
                )
                own[s, :, pl.ds(h * LANES, LANES)] = plane
                gathered[sub_at * subs + s, :, pl.ds(h * LANES, LANES)] = plane
            for k in range(len(peers)):
                plane_copy(s, k).start()

    for step in range(STEPS):
        for way in range(2):
            every = (first if step == 0 else second).at[:, pl.ds(2, 2), :, pl.ds(PAD, cells), :]
            pltpu.make_async_remote_copy(
                src_ref=every,
                dst_ref=every,
                send_sem=send_sem.at[step, way],
                recv_sem=recv_sem.at[step, way, 0],
                device_id={"gx": right},
                device_id_type=pl.DeviceIdType.MESH,
            ).wait_send()

    for s in range(subs):
        for k in range(len(peers)):
            plane_copy(s, k).wait_recv()
    for s in range(subs):
        partner = partner_table[sub_at * subs + s]
        shared_ref[s] = jnp.maximum(own[s], gathered[partner])
    for s in range(subs):
        for k in range(len(peers)):
            plane_copy(s, k).wait_send()


def put_out(final, shared, final_out, shared_out, final_sem, shared_sem):
    subs, rows = final.shape[:2]
    pieces = final_sem.shape[1]
    count = rows // pieces
    copies = [pltpu.make_async_copy(shared, shared_out, shared_sem)]
    for s in range(subs):
        for k in range(pieces):
            at = (s, pl.ds(k * count, count))
            copies.append(pltpu.make_async_copy(final.at[at], final_out.at[at], final_sem.at[s, k]))
    for copy in copies:
        copy.start()
    for copy in copies:
        copy.wait()


def on_device(dims, value_field, speed_field, drift_matrix, *others):
    subs, rows, cells, halves, sub_count, ring, total_rows = dims
    chunks = subs * BLOCKS
    in_vmem = pl.BlockSpec(memory_space=pltpu.VMEM)
    held = pltpu.VMEM((subs, rows + 4, halves, cells + 3 * PAD, LANES), jnp.float32)
    whole = pltpu.VMEM((subs, rows, halves, cells + PAD, LANES), jnp.float32)
    arrays = (value_field, speed_field, jnp.transpose(drift_matrix, (1, 0, 2)), *others)
    results = pl.pallas_call(
        functools.partial(kernel, dims),
        out_shape=(
            jax.ShapeDtypeStruct((subs, rows, cells, halves * LANES), jnp.float32),
            jax.ShapeDtypeStruct((subs, rows, cells), jnp.float32),
        ),
        in_specs=[pl.BlockSpec(memory_space=pltpu.HBM)] * 7,
        out_specs=(in_vmem, in_vmem),
        scratch_shapes=[
            held,
            held,
            whole,
            pltpu.SMEM((3, subs, 3), jnp.float32),
            pltpu.SMEM((subs, 3), jnp.float32),
            pltpu.SMEM((subs, 3), jnp.float32),
            pltpu.SMEM((sub_count * subs,), jnp.int32),
            pltpu.SMEM((subs,), jnp.int32),
            pltpu.VMEM((subs, rows, halves, 8, LANES), jnp.float32),
            pltpu.VMEM((subs, cells, LANES), jnp.float32),
            pltpu.VMEM((subs, rows, cells), jnp.float32),
            pltpu.VMEM((sub_count * subs, rows, cells), jnp.float32),
            pltpu.SemaphoreType.DMA((4, halves)),
            pltpu.SemaphoreType.DMA((5,)),
            pltpu.SemaphoreType.DMA((STEPS, 2)),
            pltpu.SemaphoreType.DMA((STEPS, 2, chunks)),
            pltpu.SemaphoreType.DMA((subs, sub_count - 1)),
            pltpu.SemaphoreType.DMA((subs, sub_count - 1)),
            pltpu.SemaphoreType.REGULAR,
        ],
        compiler_params=pltpu.CompilerParams(
            collective_id=0, has_side_effects=True, vmem_limit_bytes=40 * 1024 * 1024
        ),
        name="steps_and_planes",
    )(*(pltpu.with_memory_space_constraint(a, pltpu.HBM) for a in arrays))
    return pl.pallas_call(
        put_out,
        out_shape=tuple(jax.ShapeDtypeStruct(r.shape, r.dtype) for r in results),
        in_specs=[pl.BlockSpec(memory_space=pl.ANY)] * 2,
        out_specs=(pl.BlockSpec(memory_space=pl.ANY),) * 2,
        scratch_shapes=[pltpu.SemaphoreType.DMA((subs, 4)), pltpu.SemaphoreType.DMA],
        compiler_params=pltpu.CompilerParams(vmem_limit_bytes=1024 * 1024),
        name="put_out",
    )(*results)


def solution(mesh):
    sub_count, ring = mesh.shape["sub"], mesh.shape["gx"]

    def whole(value_field, *others):
        total_subs, total_rows, cells, third = value_field.shape
        dims = (
            total_subs // sub_count,
            total_rows // ring,
            cells,
            third // LANES,
            sub_count,
            ring,
            total_rows,
        )
        step = jax.shard_map(
            functools.partial(on_device, dims),
            mesh=mesh,
            in_specs=(
                P("sub", "gx", None, None),
                P("sub", "gx", None, None),
                P("sub", None, None),
                P("sub", None),
                P("sub", None),
                P(),
                P("sub"),
            ),
            out_specs=(P("sub", "gx", None, None), P("sub", "gx", None)),
            check_vma=False,
        )
        return step(value_field, *others)

    return whole
```
